8 devices in a mesh: dp: 1 (over z), heads: 2 (over y), ctx: 4 (over x, core).
Axes of the slice: x: 2, y: 2, z: 1, core: 2. Of those that a mesh axis runs over, the one named last changes fastest.
Arguments:
- hidden: bfloat16 [256, 2304], P(('dp', 'ctx'))
- w_query: bfloat16 [2304, 2048], P(None, 'heads')
- w_key: bfloat16 [2304, 1024], P(None, 'heads')
- w_value: bfloat16 [2304, 1024], P(None, 'heads')
- w_out: bfloat16 [2048, 2304], P('heads')
- prefix_k: bfloat16 [4096, 4, 256], P(('dp', 'ctx'), 'heads')
- prefix_v: bfloat16 [4096, 4, 256], P(('dp', 'ctx'), 'heads')
- suffix_k: bfloat16 [256, 512, 4, 256], P(('dp', 'ctx'), None, 'heads')
- suffix_v: bfloat16 [256, 512, 4, 256], P(('dp', 'ctx'), None, 'heads')
- seq_lens: int32 [256], P(('dp', 'ctx'))
Outputs:
- output: bfloat16 [256, 2304], P(('dp', 'ctx'))
All inputs are finite; a program needn't handle non-finite values.
Results may differ from the reference program's by a relative error of at most 0.00434775.
Values are sent between devices in bfloat16 or wider.
A program may use at most 1 GiB of HBM per device.

```python
import math
import jax
import jax.numpy as jnp
from jax import lax

D = 2304
HEADS = 8
KV_HEADS = 4
HEAD = 256
SEQS = 256
PREFIX = 4096
SUFFIX = 512
SEG_LEN = 1024


def draw_lens(lens_key):
    raw_lens = jax.random.randint(lens_key, (SEQS,), 0, SUFFIX, jnp.int32)
    row_ids = jnp.arange(SEQS)
    return jnp.where(row_ids == 0, SUFFIX - 1, jnp.where(row_ids == 1, 0, raw_lens)).astype(jnp.int32)


def setup_inputs(seed: int = 0, part: int = 0) -> dict:
    base_key = jax.random.key(seed)
    shared = jax.random.split(base_key, 4)
    own_keys = jax.random.split(jax.random.fold_in(base_key, part), 8)
    q_width = HEADS * HEAD
    kv_width = KV_HEADS * HEAD
    log_mass = math.log(PREFIX) + 4.0
    n_seg = PREFIX // SEG_LEN
    w_query = jax.random.normal(shared[0], (D, q_width), jnp.float32) * D ** -0.5
    w_key = jax.random.normal(shared[1], (D, kv_width), jnp.float32) * (log_mass * D ** -0.5)
    w_value = jax.random.normal(shared[2], (D, kv_width), jnp.float32) * D ** -0.5
    w_out = jax.random.normal(shared[3], (q_width, D), jnp.float32) * q_width ** -0.5
    hidden = jax.random.normal(own_keys[0], (SEQS, D), jnp.float32)
    seg_dir = jax.random.normal(own_keys[1], (n_seg, 1, KV_HEADS, HEAD), jnp.float32)
    key_noise = jax.random.normal(own_keys[2], (n_seg, SEG_LEN, KV_HEADS, HEAD), jnp.float32)
    seg_val = jax.random.normal(own_keys[3], (n_seg, 1, KV_HEADS, HEAD), jnp.float32)
    val_noise = jax.random.normal(own_keys[4], (n_seg, SEG_LEN, KV_HEADS, HEAD), jnp.float32)
    prefix_k = (key_noise + 2.0 * seg_dir).reshape(PREFIX, KV_HEADS, HEAD)
    prefix_v = (val_noise + seg_val).reshape(PREFIX, KV_HEADS, HEAD)
    suffix_k = jax.random.normal(own_keys[5], (SEQS, SUFFIX, KV_HEADS, HEAD), jnp.float32) * (log_mass / 2.5)
    suffix_v = jax.random.normal(own_keys[6], (SEQS, SUFFIX, KV_HEADS, HEAD), jnp.float32)
    seq_lens = draw_lens(own_keys[7])
    return {'hidden': hidden.astype(jnp.bfloat16), 'w_query': w_query.astype(jnp.bfloat16), 'w_key': w_key.astype(jnp.bfloat16), 'w_value': w_value.astype(jnp.bfloat16), 'w_out': w_out.astype(jnp.bfloat16), 'prefix_k': prefix_k.astype(jnp.bfloat16), 'prefix_v': prefix_v.astype(jnp.bfloat16), 'suffix_k': suffix_k.astype(jnp.bfloat16), 'suffix_v': suffix_v.astype(jnp.bfloat16), 'seq_lens': seq_lens}


def reference(hidden, w_query, w_key, w_value, w_out, prefix_k, prefix_v, suffix_k, suffix_v, seq_lens):
    q_group = HEADS // KV_HEADS
    score_scale = HEAD ** -0.5
    queries = jnp.dot(hidden, w_query, preferred_element_type=jnp.float32).astype(jnp.bfloat16).reshape(SEQS, KV_HEADS, q_group, HEAD)
    key_new = jnp.dot(hidden, w_key, preferred_element_type=jnp.float32).astype(jnp.bfloat16).reshape(SEQS, KV_HEADS, HEAD)
    val_new = jnp.dot(hidden, w_value, preferred_element_type=jnp.float32).astype(jnp.bfloat16).reshape(SEQS, KV_HEADS, HEAD)
    pre_k = prefix_k.astype(jnp.float32)
    pre_v = prefix_v.astype(jnp.float32)
    slot_ids = jnp.arange(SUFFIX)

    def one_seq(seq_item):
        q_row, k_row, v_row, cache_k, cache_v, length = seq_item
        at_slot = (slot_ids == length)[:, None, None]
        suf_keys = jnp.where(at_slot, k_row[None], cache_k).astype(jnp.float32)
        suf_vals = jnp.where(at_slot, v_row[None], cache_v).astype(jnp.float32)
        q_float = q_row.astype(jnp.float32)
        score_pre = jnp.einsum('kgd,pkd->kgp', q_float, pre_k) * score_scale
        score_suf = jnp.einsum('kgd,skd->kgs', q_float, suf_keys) * score_scale
        score_suf = jnp.where(slot_ids <= length, score_suf, -jnp.inf)
        row_max = jnp.maximum(jnp.max(score_pre, axis=-1), jnp.max(score_suf, axis=-1))[..., None]
        exp_pre = jnp.exp(score_pre - row_max)
        exp_suf = jnp.exp(score_suf - row_max)
        denominator = jnp.sum(exp_pre, axis=-1) + jnp.sum(exp_suf, axis=-1)
        numerator = jnp.einsum('kgp,pkd->kgd', exp_pre.astype(jnp.bfloat16).astype(jnp.float32), pre_v) + jnp.einsum('kgs,skd->kgd', exp_suf.astype(jnp.bfloat16).astype(jnp.float32), suf_vals)
        return (numerator / denominator[..., None]).astype(jnp.bfloat16).reshape(HEADS * HEAD)

    attended = lax.map(one_seq, (queries, key_new, val_new, suffix_k, suffix_v, seq_lens))
    mixed_out = jnp.dot(attended, w_out, preferred_element_type=jnp.float32)
    return (hidden.astype(jnp.float32) + mixed_out).astype(jnp.bfloat16)
```

```python
import functools
import math
import jax
import jax.numpy as jnp
from jax import lax
from jax.experimental import pallas as pl
from jax.experimental.pallas import tpu as pltpu
from jax.sharding import PartitionSpec as P

F32 = jnp.float32
BF16 = jnp.bfloat16
NEG = -3.0e38
RING = 24
MESH = pl.DeviceIdType.MESH
CONTRACT_LAST = (((1,), (1,)), ((), ()))


def step_kernel(x_hbm, wq_hbm, wk_hbm, wv_hbm, wo_hbm, pk_hbm, pv_hbm, sk_hbm, sv_hbm, lens_ref, y_ref,
                x, wq, wk, wv, wo, pk, pv, pve, pvo, kring, vring, qs, qrecv, qrow, snew, vnew,
                tbuf, pbuf, opart, orecv, osuf, msuf, lsuf, att, yown, yrecv,
                wsem, ksem, vsem, qsend, qrecvs, osend, orecvs, ysend, yrecvs):
    nb, width = x.shape
    slots = sk_hbm.shape[1]
    hd = 256
    rows = 2 * slots
    prows = pk.shape[1]
    factor = hd ** -0.5 * math.log2(math.e)
    groups = 4
    gsz = nb // groups
    me = lax.axis_index('ctx')
    sib = me + 1 - 2 * lax.rem(me, 2)
    far = lax.rem(me + 2, 4)
    cross = lax.rem(sib + 2, 4)
    peers = (me, sib, far, cross)
    head = lax.axis_index('heads')

    sk = sk_hbm.reshape(nb, rows, hd)
    sv = sv_hbm.reshape(nb, rows, hd)
    pkr = pk_hbm.reshape(prows, hd)
    pvr = pv_hbm.reshape(prows, hd)

    weight_copies = [
        pltpu.make_async_copy(x_hbm, x, wsem.at[0]),
        pltpu.make_async_copy(wq_hbm, wq, wsem.at[1]),
        pltpu.make_async_copy(wk_hbm, wk, wsem.at[2]),
        pltpu.make_async_copy(wv_hbm, wv, wsem.at[3]),
        pltpu.make_async_copy(wo_hbm, wo, wsem.at[4]),
    ]
    pk_copies = [pltpu.make_async_copy(pkr.at[:, pl.ds(d * 128, 128)], pk.at[d], wsem.at[5]) for d in range(2)]
    pv_copies = [pltpu.make_async_copy(pvr.at[:, pl.ds(d * 128, 128)], pv.at[d], wsem.at[6]) for d in range(2)]

    def kcopies(i, slot):
        return [pltpu.make_async_copy(sk.at[i, :, pl.ds(d * 128, 128)], kring.at[slot, d], ksem.at[slot]) for d in range(2)]

    def vcopies(i, slot):
        return [pltpu.make_async_copy(sv.at[i, :, pl.ds(d * 128, 128)], vring.at[slot, d], vsem.at[slot]) for d in range(2)]

    def start(copies):
        for c in copies:
            c.start()

    def finish(copies):
        for c in copies:
            c.wait()

    start(weight_copies[:4])
    start(pk_copies)
    start(pv_copies)

    barrier = pltpu.get_barrier_semaphore()
    for peer in peers[1:]:
        pl.semaphore_signal(barrier, inc=1, device_id={'ctx': peer}, device_id_type=MESH)
    pl.semaphore_signal(barrier, inc=1, device_id={'heads': 1 - head}, device_id_type=MESH)
    pl.semaphore_wait(barrier, 4)

    weight_copies[0].wait()
    weight_copies[1].wait()
    q = jnp.dot(x[...], wq[...], preferred_element_type=F32).astype(BF16)
    for j in range(4):
        qs[pl.ds(j * nb, nb), :] = q[:, j * hd:(j + 1) * hd]
    qf = q.astype(F32)

    q_copies = [pltpu.make_async_remote_copy(src_ref=qs, dst_ref=qrecv.at[r - 1], send_sem=qsend.at[r - 1], recv_sem=qrecvs.at[r - 1],
                                             device_id={'ctx': peers[r]}, device_id_type=MESH) for r in (1, 2, 3)]
    q_copies[1].start()
    q_copies[2].start()
    q_copies[0].start()

    for i in range(RING):
        start(kcopies(i, i))
        start(vcopies(i, i))
    weight_copies[4].start()

    for j in range(4):
        for d in range(2):
            qrow[d, pl.ds(j, nb, stride=4), :] = qf[:, j * hd + d * 128:j * hd + (d + 1) * 128]

    weight_copies[2].wait()
    weight_copies[3].wait()
    kf = jnp.dot(x[...], wk[...], preferred_element_type=F32).astype(BF16).astype(F32)
    vnew[...] = jnp.dot(x[...], wv[...], preferred_element_type=F32).astype(BF16).astype(F32)
    for j in range(4):
        prod = qf[:, j * hd:(j + 1) * hd] * kf[:, (j // 2) * hd:(j // 2 + 1) * hd]
        snew[j] = jnp.broadcast_to(jnp.sum(prod, axis=1, keepdims=True), (nb, 128))

    finish(pv_copies)
    odd_row = lax.rem(lax.broadcasted_iota(jnp.int32, (prows, 128), 0), 2).astype(F32).astype(BF16)
    even_row = 1 - odd_row
    for d in range(2):
        pve[:, pl.ds(d * 128, 128)] = pv[d] * even_row
        pvo[:, pl.ds(d * 128, 128)] = pv[d] * odd_row
    finish(pk_copies)

    lane = lax.broadcasted_iota(jnp.int32, (nb, 128), 1)
    even128 = lax.rem(lax.broadcasted_iota(jnp.int32, (2 * nb, 128), 1), 2) == 0
    even256 = lax.rem(lax.broadcasted_iota(jnp.int32, (2 * nb, 256), 1), 2) == 0

    def prefix(r):
        qv = qs[...] if r == 0 else qrecv[r - 1]
        mx = None
        for n in range(prows // 256):
            kt = jnp.concatenate([pk[0, pl.ds(n * 256, 256), :], pk[1, pl.ds(n * 256, 256), :]], axis=1)
            s = lax.dot_general(qv, kt, CONTRACT_LAST, preferred_element_type=F32)
            t = jnp.where(even256, s[:2 * nb], s[2 * nb:])
            tbuf[:, pl.ds(n * 256, 256)] = t
            top = jnp.maximum(t[:, :128], t[:, 128:])
            mx = top if mx is None else jnp.maximum(mx, top)
        m_even = jnp.max(jnp.where(even128, mx, NEG), axis=1, keepdims=True)
        m_odd = jnp.max(jnp.where(even128, NEG, mx), axis=1, keepdims=True)
        mv = jnp.where(even128, m_even, m_odd)
        tot = None
        for n in range(prows // 128):
            p = jnp.exp2((tbuf[:, pl.ds(n * 128, 128)] - mv) * factor)
            tot = p if tot is None else tot + p
            pbuf[:, pl.ds(n * 128, 128)] = p.astype(BF16)
        l_even = jnp.sum(jnp.where(even128, tot, 0.0), axis=1, keepdims=True)
        l_odd = jnp.sum(jnp.where(even128, 0.0, tot), axis=1, keepdims=True)
        stats = jnp.zeros((nb, 128), F32)
        for h, (vals, m, l) in enumerate(((pve, m_even, l_even), (pvo, m_odd, l_odd))):
            o = jnp.dot(pbuf[...], vals[...], preferred_element_type=F32)
            for g in range(2):
                j = 2 * h + g
                opart[r, :, pl.ds(j * hd, hd)] = o[g * nb:(g + 1) * nb]
                stats = jnp.where(lane == 2 * j, m[g * nb:(g + 1) * nb], stats)
                stats = jnp.where(lane == 2 * j + 1, l[g * nb:(g + 1) * nb], stats)
        opart[r, :, pl.ds(4 * hd, 128)] = stats

    def o_copy(r, g):
        part = pl.ds(g * gsz, gsz)
        return pltpu.make_async_remote_copy(src_ref=opart.at[r, part], dst_ref=orecv.at[r - 1, part], send_sem=osend.at[r - 1, g],
                                            recv_sem=orecvs.at[r - 1, g], device_id={'ctx': peers[r]}, device_id_type=MESH)

    row8 = lax.broadcasted_iota(jnp.int32, (8, rows), 0)
    col = lax.broadcasted_iota(jnp.int32, (8, rows), 1)
    same_head = lax.rem(col, 2) == lax.rem(row8 // 2, 2)
    slot_of = jnp.where(same_head, col // 2, 1 << 20)
    first = row8 < 4
    first128 = lax.broadcasted_iota(jnp.int32, (8, 128), 0) < 4
    first256 = lax.broadcasted_iota(jnp.int32, (8, 256), 0) < 4

    def scores(i):
        at = pl.multiple_of(i * 4, 8)
        q8 = jnp.concatenate([qrow[0, pl.ds(at, 8), :], qrow[1, pl.ds(at, 8), :]], axis=1).astype(BF16)
        out = []
        for u in range(2):
            slot = lax.rem(i + u, RING)
            kk = jnp.concatenate([kring[slot, 0], kring[slot, 1]], axis=1)
            out.append(lax.dot_general(q8, kk, CONTRACT_LAST, preferred_element_type=F32))
        return jnp.where(first, out[0], out[1])

    def values(i, s):
        at = pl.multiple_of(i * 4, 8)
        ln = jnp.where(first128, lens_ref[i], lens_ref[i + 1])
        ln = jnp.concatenate([ln] * (rows // 128), axis=1)
        s = jnp.where(slot_of < ln, s, NEG)
        m = jnp.max(s, axis=1, keepdims=True)
        p = jnp.exp2((s - m) * factor)
        l = jnp.sum(p, axis=1, keepdims=True)
        pb = p.astype(BF16)
        out = []
        for u in range(2):
            slot = lax.rem(i + u, RING)
            vv = jnp.concatenate([vring[slot, 0], vring[slot, 1]], axis=1)
            out.append(jnp.dot(pb, vv, preferred_element_type=F32))
        o = jnp.where(first256, out[0], out[1])
        osuf[0, pl.ds(at, 8), :] = o[:, :128]
        osuf[1, pl.ds(at, 8), :] = o[:, 128:]
        msuf[pl.ds(at, 8), :] = jnp.broadcast_to(m, (8, 128))
        lsuf[pl.ds(at, 8), :] = jnp.broadcast_to(l, (8, 128))

    def suffix(lo, hi, per=4):
        refill = lo + RING < nb

        def wait_k(i):
            for u in range(per):
                finish(kcopies(i + u, lax.rem(i + u, RING)))

        def wait_v(i):
            for u in range(per):
                finish(vcopies(i + u, lax.rem(i + u, RING)))

        def fill(i):
            if refill:
                for u in range(per):
                    start(kcopies(i + u + RING, lax.rem(i + u, RING)))
                    start(vcopies(i + u + RING, lax.rem(i + u, RING)))

        def body(it, ss):
            i = lo + it * per
            wait_k(i + per)
            wait_v(i)
            nxt = tuple(scores(i + per + 2 * u) for u in range(per // 2))
            for u in range(per // 2):
                values(i + 2 * u, ss[u])
            fill(i)
            return nxt

        wait_k(lo)
        ss = tuple(scores(lo + 2 * u) for u in range(per // 2))
        ss = lax.fori_loop(0, (hi - lo) // per - 1, body, ss)
        last = hi - per
        wait_v(last)
        for u in range(per // 2):
            values(last + 2 * u, ss[u])
        fill(last)

    def y_copy(g):
        part = pl.ds(g * gsz, gsz)
        return pltpu.make_async_remote_copy(src_ref=yown.at[part], dst_ref=yrecv.at[part], send_sem=ysend.at[g], recv_sem=yrecvs.at[g],
                                            device_id={'heads': 1 - head}, device_id_type=MESH)

    def merge(g):
        for r in (1, 2, 3):
            o_copy(r, g).wait_recv()
        part = pl.ds(g * gsz, gsz)
        srcs = [opart.at[0], orecv.at[0], orecv.at[1], orecv.at[2]]
        for j in range(4):
            rows_j = pl.ds(g * gsz * 4 + j, gsz, stride=4)
            ms = [msuf[rows_j, :], snew[j, part, :]]
            for src in srcs:
                ms.append(jnp.broadcast_to(src[part, pl.ds(4 * hd + 2 * j, 1)], (gsz, 128)))
            top = functools.reduce(jnp.maximum, ms)
            ws = [jnp.exp2((m - top) * factor) for m in ms]
            den = ws[0] * lsuf[rows_j, :] + ws[1]
            for w, src in zip(ws[2:], srcs):
                den = den + w * src[part, pl.ds(4 * hd + 2 * j + 1, 1)]
            for d in range(2):
                at = j * hd + d * 128
                num = ws[0] * osuf[d, rows_j, :] + ws[1] * vnew[part, pl.ds((j // 2) * hd + d * 128, 128)]
                for w, src in zip(ws[2:], srcs):
                    num = num + w * src[part, pl.ds(at, 128)]
                att[:, pl.ds(at, 128)] = (num / den).astype(BF16)
        yown[part, :] = jnp.dot(att[...], wo[...], preferred_element_type=F32)
        y_copy(g).start()

    prefix(0)
    suffix(0, 8)
    q_copies[1].wait_recv()
    prefix(2)
    o_copy(2, 0).start()
    q_copies[2].wait_recv()
    prefix(3)
    o_copy(3, 0).start()
    for g in range(1, groups):
        o_copy(2, g).start()
        o_copy(3, g).start()
    q_copies[0].wait_recv()
    prefix(1)
    for g in range(groups):
        o_copy(1, g).start()
    suffix(8, 24)
    suffix(24, 40)
    weight_copies[4].wait()
    merge(0)
    merge(1)
    suffix(40, 64)
    merge(2)
    merge(3)
    for c in q_copies:
        c.wait_send()
    for r in (1, 2, 3):
        for g in range(groups):
            o_copy(r, g).wait_send()
    for g in range(groups):
        part = pl.ds(g * gsz, gsz)
        y_copy(g).wait()
        y_ref[part, :] = (x[part, :].astype(F32) + (yown[part, :] + yrecv[part, :])).astype(BF16)


def solution(mesh):
    row_spec = P(('dp', 'ctx'), None)
    col_spec = P(None, 'heads')
    pre_spec = P(('dp', 'ctx'), 'heads', None)
    suf_spec = P(('dp', 'ctx'), None, 'heads', None)

    def local_step(hidden, w_query, w_key, w_value, w_out, prefix_k, prefix_v, suffix_k, suffix_v, seq_lens):
        nb, width = hidden.shape
        qw = w_query.shape[1]
        kvw = w_key.shape[1]
        prows = 2 * prefix_k.shape[0]
        rows = 2 * suffix_k.shape[1]
        any_spec = pl.BlockSpec(memory_space=pl.ANY)
        dma = pltpu.SemaphoreType.DMA
        v = pltpu.VMEM
        return pl.pallas_call(
            step_kernel,
            out_shape=jax.ShapeDtypeStruct((nb, width), BF16),
            in_specs=[any_spec] * 9 + [pl.BlockSpec(memory_space=pltpu.SMEM)],
            out_specs=pl.BlockSpec(memory_space=pltpu.VMEM),
            scratch_shapes=[
                v((nb, width), BF16), v((width, qw), BF16), v((width, kvw), BF16), v((width, kvw), BF16), v((qw, width), BF16),
                v((2, prows, 128), BF16), v((2, prows, 128), BF16), v((prows, 256), BF16), v((prows, 256), BF16),
                v((RING, 2, rows, 128), BF16), v((RING, 2, rows, 128), BF16),
                v((4 * nb, 256), BF16), v((3, 4 * nb, 256), BF16), v((2, 4 * nb, 128), F32), v((4, nb, 128), F32), v((nb, kvw), F32),
                v((2 * nb, prows), F32), v((2 * nb, prows), BF16),
                v((4, nb, qw + 128), F32), v((3, nb, qw + 128), F32),
                v((2, 4 * nb, 128), F32), v((4 * nb, 128), F32), v((4 * nb, 128), F32), v((nb // 4, qw), BF16),
                v((nb, width), F32), v((nb, width), F32),
                dma((7,)), dma((RING,)), dma((RING,)), dma((3,)), dma((3,)), dma((3, 4)), dma((3, 4)), dma((4,)), dma((4,)),
            ],
            compiler_params=pltpu.CompilerParams(collective_id=0, has_side_effects=True, vmem_limit_bytes=60 * 1024 * 1024),
        )(hidden, w_query, w_key, w_value, w_out, prefix_k, prefix_v, suffix_k, suffix_v, seq_lens)

    return jax.shard_map(local_step, mesh=mesh, in_specs=(row_spec, col_spec, col_spec, col_spec, P('heads', None), pre_spec, pre_spec, suf_spec, suf_spec, P(('dp', 'ctx'))), out_specs=row_spec, check_vma=False)
```

```python
import functools
import math
import jax
import jax.numpy as jnp
from jax import lax
from jax.experimental import pallas as pl
from jax.experimental.pallas import tpu as pltpu
from jax.sharding import PartitionSpec as P

F32 = jnp.float32
BF16 = jnp.bfloat16
NEG = -3.0e38
PER = 4
RING = 6
GROUPS = ((0, 16), (16, 40), (40, 56), (56, 64))
SPLIT = 3
MESH = pl.DeviceIdType.MESH
CONTRACT_LAST = (((1,), (1,)), ((), ()))


def step_kernel(x_hbm, wq_hbm, wk_hbm, wv_hbm, wo_hbm, pk_hbm, pv_hbm, sk_hbm, sv_hbm, lens_hbm, y_ref,
                x, wq, wk, wv, wo, pk, pv, pve, pvo, kring, vring, qs, qrecv, qrow, snew, vnew,
                tbuf, pbuf, opart, orecv, osuf, msuf, lsuf, att, yown, yrecv, yfin, lens_ref,
                wsem, ksem, vsem, psend, precv, qsend, qrecvs, osend, orecvs, ysend, yrecvs, fsend, frecv):
    nb, width = x.shape
    slots = sk_hbm.shape[1]
    hd = 256
    rows = 2 * slots
    prows = pk.shape[2]
    factor = hd ** -0.5 * math.log2(math.e)
    me = lax.axis_index('ctx')
    sib = me + 1 - 2 * lax.rem(me, 2)
    far = lax.rem(me + 2, 4)
    head = lax.axis_index('heads')

    sk = sk_hbm.reshape(nb, rows, hd)
    sv = sv_hbm.reshape(nb, rows, hd)
    pkr = pk_hbm.reshape(prows, hd)
    pvr = pv_hbm.reshape(prows, hd)

    third = width // 3
    x_copy = pltpu.make_async_copy(x_hbm, x, wsem.at[0])
    lens_copy = pltpu.make_async_copy(lens_hbm, lens_ref, wsem.at[9])
    wq_copies = [pltpu.make_async_copy(wq_hbm.at[pl.ds(c * third, third)], wq.at[pl.ds(c * third, third)], wsem.at[1 + c]) for c in range(3)]
    wk_copy = pltpu.make_async_copy(wk_hbm, wk, wsem.at[4])
    wv_copy = pltpu.make_async_copy(wv_hbm, wv, wsem.at[5])
    wo_copy = pltpu.make_async_copy(wo_hbm, wo, wsem.at[6])
    pk_copies = [pltpu.make_async_copy(pkr.at[:, pl.ds(d * 128, 128)], pk.at[0, d], wsem.at[7]) for d in range(2)]
    pv_copies = [pltpu.make_async_copy(pvr.at[:, pl.ds(d * 128, 128)], pv.at[0, d], wsem.at[8]) for d in range(2)]

    def to_sibling(buf, n):
        return pltpu.make_async_remote_copy(src_ref=buf.at[0], dst_ref=buf.at[1], send_sem=psend.at[n], recv_sem=precv.at[n],
                                            device_id={'ctx': sib}, device_id_type=MESH)

    pk_share = to_sibling(pk, 0)
    pv_share = to_sibling(pv, 1)

    def kcopies(n):
        slot = lax.rem(n, RING)
        return [pltpu.make_async_copy(sk.at[pl.ds(n * PER, PER), :, pl.ds(d * 128, 128)], kring.at[slot, d], ksem.at[slot]) for d in range(2)]

    def vcopies(n):
        slot = lax.rem(n, RING)
        return [pltpu.make_async_copy(sv.at[pl.ds(n * PER, PER), :, pl.ds(d * 128, 128)], vring.at[slot, d], vsem.at[slot]) for d in range(2)]

    def start(copies):
        for c in copies:
            c.start()

    def finish(copies):
        for c in copies:
            c.wait()

    x_copy.start()
    lens_copy.start()
    start(wq_copies)

    barrier = pltpu.get_barrier_semaphore()
    pl.semaphore_signal(barrier, inc=1, device_id={'ctx': sib}, device_id_type=MESH)
    pl.semaphore_signal(barrier, inc=1, device_id={'ctx': far}, device_id_type=MESH)
    pl.semaphore_signal(barrier, inc=1, device_id={'heads': 1 - head}, device_id_type=MESH)
    start(pk_copies)
    start(pv_copies)
    wk_copy.start()
    wv_copy.start()
    pl.semaphore_wait(barrier, 3)

    x_copy.wait()
    q = None
    for c in range(3):
        wq_copies[c].wait()
        if c == 2:
            start(kcopies(0))
            start(vcopies(0))
        piece = jnp.dot(x[:, pl.ds(c * third, third)], wq[pl.ds(c * third, third), :], preferred_element_type=F32)
        q = piece if q is None else q + piece
    q = q.astype(BF16)
    for j in range(4):
        qs[pl.ds(j * nb, nb), :] = q[:, j * hd:(j + 1) * hd]
    qf = q.astype(F32)

    q_copy = pltpu.make_async_remote_copy(src_ref=qs, dst_ref=qrecv, send_sem=qsend.at[0], recv_sem=qrecvs.at[0],
                                          device_id={'ctx': far}, device_id_type=MESH)
    q_copy.start()
    finish(pk_copies)
    pk_share.start()
    finish(pv_copies)
    pv_share.start()

    for i in range(1, RING):
        start(kcopies(i))
        start(vcopies(i))
    wo_copy.start()

    for j in range(4):
        for d in range(2):
            qrow[d, pl.ds(j, nb, stride=4), :] = qf[:, j * hd + d * 128:j * hd + (d + 1) * 128]

    wk_copy.wait()
    wv_copy.wait()
    kf = jnp.dot(x[...], wk[...], preferred_element_type=F32).astype(BF16).astype(F32)
    vnew[...] = jnp.dot(x[...], wv[...], preferred_element_type=F32).astype(BF16).astype(F32)
    for j in range(4):
        prod = qf[:, j * hd:(j + 1) * hd] * kf[:, (j // 2) * hd:(j // 2 + 1) * hd]
        snew[j] = jnp.broadcast_to(jnp.sum(prod, axis=1, keepdims=True), (nb, 128))

    odd_row = lax.rem(lax.broadcasted_iota(jnp.int32, (prows, 128), 0), 2).astype(F32).astype(BF16)
    even_row = 1 - odd_row

    def split_values(c):
        for d in range(2):
            pve[pl.ds(c * prows, prows), pl.ds(d * 128, 128)] = pv[c, d] * even_row
            pvo[pl.ds(c * prows, prows), pl.ds(d * 128, 128)] = pv[c, d] * odd_row

    split_values(0)

    lane = lax.broadcasted_iota(jnp.int32, (nb, 128), 1)
    even128 = lax.rem(lax.broadcasted_iota(jnp.int32, (2 * nb, 128), 1), 2) == 0
    even256 = lax.rem(lax.broadcasted_iota(jnp.int32, (2 * nb, 256), 1), 2) == 0

    def prefix(r):
        qv = qrecv[...] if r else qs[...]
        mx = None
        for n in range(2 * prows // 256):
            c, at = divmod(n * 256, prows)
            kt = jnp.concatenate([pk[c, 0, pl.ds(at, 256), :], pk[c, 1, pl.ds(at, 256), :]], axis=1)
            s = lax.dot_general(qv, kt, CONTRACT_LAST, preferred_element_type=F32)
            t = jnp.where(even256, s[:2 * nb], s[2 * nb:])
            tbuf[:, pl.ds(n * 256, 256)] = t
            top = jnp.maximum(t[:, :128], t[:, 128:])
            mx = top if mx is None else jnp.maximum(mx, top)
        m_even = jnp.max(jnp.where(even128, mx, NEG), axis=1, keepdims=True)
        m_odd = jnp.max(jnp.where(even128, NEG, mx), axis=1, keepdims=True)
        mv = jnp.where(even128, m_even, m_odd)
        tot = None
        for n in range(2 * prows // 128):
            p = jnp.exp2((tbuf[:, pl.ds(n * 128, 128)] - mv) * factor)
            tot = p if tot is None else tot + p
            pbuf[:, pl.ds(n * 128, 128)] = p.astype(BF16)
        l_even = jnp.sum(jnp.where(even128, tot, 0.0), axis=1, keepdims=True)
        l_odd = jnp.sum(jnp.where(even128, 0.0, tot), axis=1, keepdims=True)
        stats = jnp.zeros((nb, 128), F32)
        for h, (vals, m, l) in enumerate(((pve, m_even, l_even), (pvo, m_odd, l_odd))):
            o = jnp.dot(pbuf[...], vals[...], preferred_element_type=F32)
            for g in range(2):
                j = 2 * h + g
                opart[r, :, pl.ds(j * hd, hd)] = o[g * nb:(g + 1) * nb]
                stats = jnp.where(lane == 2 * j, m[g * nb:(g + 1) * nb], stats)
                stats = jnp.where(lane == 2 * j + 1, l[g * nb:(g + 1) * nb], stats)
        opart[r, :, pl.ds(4 * hd, 128)] = stats

    def o_copy(g):
        lo, hi = GROUPS[g]
        part = pl.ds(lo, hi - lo)
        return pltpu.make_async_remote_copy(src_ref=opart.at[1, part], dst_ref=orecv.at[part], send_sem=osend.at[g],
                                            recv_sem=orecvs.at[g], device_id={'ctx': far}, device_id_type=MESH)

    row8 = lax.broadcasted_iota(jnp.int32, (8, rows), 0)
    col = lax.broadcasted_iota(jnp.int32, (8, rows), 1)
    same_head = lax.rem(col, 2) == lax.rem(row8 // 2, 2)
    slot_of = jnp.where(same_head, col // 2, 1 << 20)
    first = row8 < 4
    first128 = lax.broadcasted_iota(jnp.int32, (8, 128), 0) < 4
    first256 = lax.broadcasted_iota(jnp.int32, (8, 256), 0) < 4

    def scores(n, pair):
        at = pl.multiple_of((n * PER + 2 * pair) * 4, 8)
        slot = lax.rem(n, RING)
        q8 = jnp.concatenate([qrow[0, pl.ds(at, 8), :], qrow[1, pl.ds(at, 8), :]], axis=1).astype(BF16)
        out = []
        for u in (2 * pair, 2 * pair + 1):
            kk = jnp.concatenate([kring[slot, 0, u], kring[slot, 1, u]], axis=1)
            out.append(lax.dot_general(q8, kk, CONTRACT_LAST, preferred_element_type=F32))
        return jnp.where(first, out[0], out[1])

    def values(n, pair, s):
        i = n * PER + 2 * pair
        at = pl.multiple_of(i * 4, 8)
        slot = lax.rem(n, RING)
        ln = jnp.where(first128, lens_ref[i], lens_ref[i + 1])
        ln = jnp.concatenate([ln] * (rows // 128), axis=1)
        s = jnp.where(slot_of < ln, s, NEG)
        m = jnp.max(s, axis=1, keepdims=True)
        p = jnp.exp2((s - m) * factor)
        l = jnp.sum(p, axis=1, keepdims=True)
        pb = p.astype(BF16)
        out = []
        for u in (2 * pair, 2 * pair + 1):
            vv = jnp.concatenate([vring[slot, 0, u], vring[slot, 1, u]], axis=1)
            out.append(jnp.dot(pb, vv, preferred_element_type=F32))
        o = jnp.where(first256, out[0], out[1])
        osuf[0, pl.ds(at, 8), :] = o[:, :128]
        osuf[1, pl.ds(at, 8), :] = o[:, 128:]
        msuf[pl.ds(at, 8), :] = jnp.broadcast_to(m, (8, 128))
        lsuf[pl.ds(at, 8), :] = jnp.broadcast_to(l, (8, 128))

    pairs = range(PER // 2)
    blocks = nb // PER

    def first_scores():
        finish(kcopies(0))
        return tuple(scores(0, p) for p in pairs)

    def suffix(lo, hi, ss):
        lo, hi = lo // PER, hi // PER
        refill = hi + RING <= blocks
        assert refill or lo + RING >= blocks

        def body(n, ss):
            if refill:
                start(kcopies(n + RING))
            finish(kcopies(n + 1))
            finish(vcopies(n))
            nxt = tuple(scores(n + 1, p) for p in pairs)
            for p in pairs:
                values(n, p, ss[p])
            if refill:
                start(vcopies(n + RING))
            return nxt

        if hi < blocks:
            return lax.fori_loop(lo, hi, body, ss)
        ss = lax.fori_loop(lo, hi - 1, body, ss)
        finish(vcopies(hi - 1))
        for p in pairs:
            values(hi - 1, p, ss[p])

    half = width // 2
    mine = pl.ds(pl.multiple_of(head * half, 128), half)
    other = pl.ds(pl.multiple_of((1 - head) * half, 128), half)

    def y_copy(g):
        lo, hi = GROUPS[g]
        part = (pl.ds(lo, hi - lo), other if g < SPLIT else slice(None))
        return pltpu.make_async_remote_copy(src_ref=yown.at[part], dst_ref=yrecv.at[part], send_sem=ysend.at[g], recv_sem=yrecvs.at[g],
                                            device_id={'heads': 1 - head}, device_id_type=MESH)

    def f_copy(g):
        lo, hi = GROUPS[g]
        part = (pl.ds(lo, hi - lo), mine)
        return pltpu.make_async_remote_copy(src_ref=yfin.at[part], dst_ref=yfin.at[part], send_sem=fsend.at[g], recv_sem=frecv.at[g],
                                            device_id={'heads': 1 - head}, device_id_type=MESH)

    def finalize(g):
        y_copy(g).wait_recv()
        lo, hi = GROUPS[g]
        part = (pl.ds(lo, hi - lo), mine)
        yfin[part] = (x[part].astype(F32) + (yown[part] + yrecv[part])).astype(BF16)
        f_copy(g).start()

    def merge(g):
        o_copy(g).wait_recv()
        lo, hi = GROUPS[g]
        gsz = hi - lo
        part = pl.ds(lo, gsz)
        srcs = [opart.at[0], orecv]
        for j in range(4):
            rows_j = pl.ds(lo * 4 + j, gsz, stride=4)
            ms = [msuf[rows_j, :], snew[j, part, :]]
            for src in srcs:
                ms.append(jnp.broadcast_to(src[part, pl.ds(4 * hd + 2 * j, 1)], (gsz, 128)))
            top = functools.reduce(jnp.maximum, ms)
            ws = [jnp.exp2((m - top) * factor) for m in ms]
            den = ws[0] * lsuf[rows_j, :] + ws[1]
            for w, src in zip(ws[2:], srcs):
                den = den + w * src[part, pl.ds(4 * hd + 2 * j + 1, 1)]
            for d in range(2):
                at = j * hd + d * 128
                num = ws[0] * osuf[d, rows_j, :] + ws[1] * vnew[part, pl.ds((j // 2) * hd + d * 128, 128)]
                for w, src in zip(ws[2:], srcs):
                    num = num + w * src[part, pl.ds(at, 128)]
                att[pl.ds(0, gsz), pl.ds(at, 128)] = (num / den).astype(BF16)
        yown[part, :] = jnp.dot(att[pl.ds(0, gsz), :], wo[...], preferred_element_type=F32)
        y_copy(g).start()

    lens_copy.wait()
    ss = first_scores()
    ss = suffix(0, 8, ss)
    pv_share.wait_recv()
    split_values(1)
    pk_share.wait_recv()
    prefix(0)
    ss = suffix(8, 16, ss)
    q_copy.wait_recv()
    prefix(1)
    for g in range(len(GROUPS)):
        o_copy(g).start()
    ss = suffix(16, 40, ss)
    wo_copy.wait()
    merge(0)
    ss = suffix(40, 48, ss)
    merge(1)
    finalize(0)
    ss = suffix(48, 56, ss)
    merge(2)
    finalize(1)
    suffix(56, 64, ss)
    merge(3)
    finalize(2)
    q_copy.wait_send()
    pk_share.wait_send()
    pv_share.wait_send()
    for g, (lo, hi) in enumerate(GROUPS):
        o_copy(g).wait_send()
        y_copy(g).wait_send()
        part = pl.ds(lo, hi - lo)
        if g < SPLIT:
            f_copy(g).wait()
            y_ref[part, :] = yfin[part, :]
        else:
            y_copy(g).wait_recv()
            y_ref[part, :] = (x[part, :].astype(F32) + (yown[part, :] + yrecv[part, :])).astype(BF16)


def solution(mesh):
    row_spec = P(('dp', 'ctx'), None)
    col_spec = P(None, 'heads')
    pre_spec = P(('dp', 'ctx'), 'heads', None)
    suf_spec = P(('dp', 'ctx'), None, 'heads', None)

    def local_step(hidden, w_query, w_key, w_value, w_out, prefix_k, prefix_v, suffix_k, suffix_v, seq_lens):
        nb, width = hidden.shape
        qw = w_query.shape[1]
        kvw = w_key.shape[1]
        prows = 2 * prefix_k.shape[0]
        rows = 2 * suffix_k.shape[1]
        hbm_spec = pl.BlockSpec(memory_space=pltpu.HBM)
        dma = pltpu.SemaphoreType.DMA
        v = pltpu.VMEM
        return pl.pallas_call(
            step_kernel,
            out_shape=jax.ShapeDtypeStruct((nb, width), BF16),
            in_specs=[hbm_spec] * 10,
            out_specs=pl.BlockSpec(memory_space=pltpu.VMEM),
            scratch_shapes=[
                v((nb, width), BF16), v((width, qw), BF16), v((width, kvw), BF16), v((width, kvw), BF16), v((qw, width), BF16),
                v((2, 2, prows, 128), BF16), v((2, 2, prows, 128), BF16), v((2 * prows, 256), BF16), v((2 * prows, 256), BF16),
                v((RING, 2, PER, rows, 128), BF16), v((RING, 2, PER, rows, 128), BF16),
                v((4 * nb, 256), BF16), v((4 * nb, 256), BF16), v((2, 4 * nb, 128), F32), v((4, nb, 128), F32), v((nb, kvw), F32),
                v((2 * nb, 2 * prows), F32), v((2 * nb, 2 * prows), BF16),
                v((2, nb, qw + 128), F32), v((nb, qw + 128), F32),
                v((2, 4 * nb, 128), F32), v((4 * nb, 128), F32), v((4 * nb, 128), F32), v((nb // 2, qw), BF16),
                v((nb, width), F32), v((nb, width), F32), v((nb, width), BF16), pltpu.SMEM((nb,), jnp.int32),
                dma((10,)), dma((RING,)), dma((RING,)), dma((2,)), dma((2,)), dma((1,)), dma((1,)), dma((4,)), dma((4,)), dma((4,)), dma((4,)), dma((4,)), dma((4,)),
            ],
            compiler_params=pltpu.CompilerParams(collective_id=0, has_side_effects=True, vmem_limit_bytes=60 * 1024 * 1024),
        )(hidden, w_query, w_key, w_value, w_out, prefix_k, prefix_v, suffix_k, suffix_v, seq_lens)

    return jax.shard_map(local_step, mesh=mesh, in_specs=(row_spec, col_spec, col_spec, col_spec, P('heads', None), pre_spec, pre_spec, suf_spec, suf_spec, P(('dp', 'ctx'))), out_specs=row_spec, check_vma=False)
```

```python
import functools
import math
import jax
import jax.numpy as jnp
from jax import lax
from jax.experimental import pallas as pl
from jax.experimental.pallas import tpu as pltpu
from jax.sharding import PartitionSpec as P

F32 = jnp.float32
BF16 = jnp.bfloat16
NEG = -3.0e38
PER = 4
RING = 6
GROUPS = ((0, 16), (16, 40), (40, 56), (56, 64))
SPLIT = 3
MESH = pl.DeviceIdType.MESH
CONTRACT_LAST = (((1,), (1,)), ((), ()))


def step_kernel(x_hbm, wq_hbm, wk_hbm, wv_hbm, wo_hbm, pk_hbm, pv_hbm, sk_hbm, sv_hbm, lens_hbm, y_ref,
                x, wq, wk, wv, wo, pk, pv, pve, pvo, kring, vring, qs, qrecv, qrow, snew, vnew,
                tbuf, pbuf, opart, orecv, osuf, msuf, lsuf, att, yown, yrecv, yfin, lens_ref,
                wsem, ksem, vsem, psend, precv, qsend, qrecvs, osend, orecvs, ysend, yrecvs, fsend, frecv):
    nb, width = x.shape
    slots = sk_hbm.shape[1]
    hd = 256
    rows = 2 * slots
    prows = pk.shape[2]
    factor = hd ** -0.5 * math.log2(math.e)
    me = lax.axis_index('ctx')
    sib = me + 1 - 2 * lax.rem(me, 2)
    far = lax.rem(me + 2, 4)
    head = lax.axis_index('heads')

    sk = sk_hbm.reshape(nb, rows, hd)
    sv = sv_hbm.reshape(nb, rows, hd)
    pkr = pk_hbm.reshape(prows, hd)
    pvr = pv_hbm.reshape(prows, hd)

    third = width // 3
    x_copy = pltpu.make_async_copy(x_hbm, x, wsem.at[0])
    lens_copy = pltpu.make_async_copy(lens_hbm, lens_ref, wsem.at[9])
    wq_copies = [pltpu.make_async_copy(wq_hbm.at[pl.ds(c * third, third)], wq.at[pl.ds(c * third, third)], wsem.at[1 + c]) for c in range(3)]
    wk_copy = pltpu.make_async_copy(wk_hbm, wk, wsem.at[4])
    wv_copy = pltpu.make_async_copy(wv_hbm, wv, wsem.at[5])
    wo_copy = pltpu.make_async_copy(wo_hbm, wo, wsem.at[6])
    pk_copies = [pltpu.make_async_copy(pkr.at[:, pl.ds(d * 128, 128)], pk.at[0, d], wsem.at[7]) for d in range(2)]
    pv_copies = [pltpu.make_async_copy(pvr.at[:, pl.ds(d * 128, 128)], pv.at[0, d], wsem.at[8]) for d in range(2)]

    def to_sibling(buf, n):
        return pltpu.make_async_remote_copy(src_ref=buf.at[0], dst_ref=buf.at[1], send_sem=psend.at[n], recv_sem=precv.at[n],
                                            device_id={'ctx': sib}, device_id_type=MESH)

    pk_share = to_sibling(pk, 0)
    pv_share = to_sibling(pv, 1)

    def kcopies(n):
        slot = lax.rem(n, RING)
        return [pltpu.make_async_copy(sk.at[pl.ds(n * PER, PER), :, pl.ds(d * 128, 128)], kring.at[slot, d], ksem.at[slot]) for d in range(2)]

    def vcopies(n):
        slot = lax.rem(n, RING)
        return [pltpu.make_async_copy(sv.at[pl.ds(n * PER, PER), :, pl.ds(d * 128, 128)], vring.at[slot, d], vsem.at[slot]) for d in range(2)]

    def start(copies):
        for c in copies:
            c.start()

    def finish(copies):
        for c in copies:
            c.wait()

    x_copy.start()
    lens_copy.start()
    start(wq_copies)

    barrier = pltpu.get_barrier_semaphore()
    pl.semaphore_signal(barrier, inc=1, device_id={'ctx': sib}, device_id_type=MESH)
    pl.semaphore_signal(barrier, inc=1, device_id={'ctx': far}, device_id_type=MESH)
    pl.semaphore_signal(barrier, inc=1, device_id={'heads': 1 - head}, device_id_type=MESH)
    start(pk_copies)
    start(pv_copies)
    wk_copy.start()
    wv_copy.start()
    pl.semaphore_wait(barrier, 3)

    x_copy.wait()
    q = None
    for c in range(3):
        wq_copies[c].wait()
        if c == 2:
            start(kcopies(0))
            start(vcopies(0))
        piece = jnp.dot(x[:, pl.ds(c * third, third)], wq[pl.ds(c * third, third), :], preferred_element_type=F32)
        q = piece if q is None else q + piece
    q = q.astype(BF16)
    for j in range(4):
        qs[pl.ds(j * nb, nb), :] = q[:, j * hd:(j + 1) * hd]
    qf = q.astype(F32)

    q_copy = pltpu.make_async_remote_copy(src_ref=qs, dst_ref=qrecv, send_sem=qsend.at[0], recv_sem=qrecvs.at[0],
                                          device_id={'ctx': far}, device_id_type=MESH)
    q_copy.start()
    finish(pk_copies)
    pk_share.start()
    finish(pv_copies)
    pv_share.start()

    for i in range(1, RING):
        start(kcopies(i))
        start(vcopies(i))
    wo_copy.start()

    for j in range(4):
        for d in range(2):
            qrow[d, pl.ds(j, nb, stride=4), :] = qf[:, j * hd + d * 128:j * hd + (d + 1) * 128]

    wk_copy.wait()
    wv_copy.wait()
    kf = jnp.dot(x[...], wk[...], preferred_element_type=F32).astype(BF16).astype(F32)
    vnew[...] = jnp.dot(x[...], wv[...], preferred_element_type=F32).astype(BF16).astype(F32)
    for j in range(4):
        prod = qf[:, j * hd:(j + 1) * hd] * kf[:, (j // 2) * hd:(j // 2 + 1) * hd]
        snew[j] = jnp.broadcast_to(jnp.sum(prod, axis=1, keepdims=True), (nb, 128))

    odd_row = lax.rem(lax.broadcasted_iota(jnp.int32, (prows, 128), 0), 2).astype(F32).astype(BF16)
    even_row = 1 - odd_row

    def split_values(c):
        for d in range(2):
            pve[pl.ds(c * prows, prows), pl.ds(d * 128, 128)] = pv[c, d] * even_row
            pvo[pl.ds(c * prows, prows), pl.ds(d * 128, 128)] = pv[c, d] * odd_row

    split_values(0)

    lane = lax.broadcasted_iota(jnp.int32, (nb, 128), 1)
    even128 = lax.rem(lax.broadcasted_iota(jnp.int32, (2 * nb, 128), 1), 2) == 0
    even256 = lax.rem(lax.broadcasted_iota(jnp.int32, (2 * nb, 256), 1), 2) == 0

    def prefix(r):
        qv = qrecv[...] if r else qs[...]
        mx = None
        for n in range(2 * prows // 256):
            c, at = divmod(n * 256, prows)
            kt = jnp.concatenate([pk[c, 0, pl.ds(at, 256), :], pk[c, 1, pl.ds(at, 256), :]], axis=1)
            s = lax.dot_general(qv, kt, CONTRACT_LAST, preferred_element_type=F32)
            t = jnp.where(even256, s[:2 * nb], s[2 * nb:])
            tbuf[:, pl.ds(n * 256, 256)] = t
            top = jnp.maximum(t[:, :128], t[:, 128:])
            mx = top if mx is None else jnp.maximum(mx, top)
        m_even = jnp.max(jnp.where(even128, mx, NEG), axis=1, keepdims=True)
        m_odd = jnp.max(jnp.where(even128, NEG, mx), axis=1, keepdims=True)
        mv = jnp.where(even128, m_even, m_odd)
        tot = None
        for n in range(2 * prows // 128):
            p = jnp.exp2((tbuf[:, pl.ds(n * 128, 128)] - mv) * factor)
            tot = p if tot is None else tot + p
            pbuf[:, pl.ds(n * 128, 128)] = p.astype(BF16)
        l_even = jnp.sum(jnp.where(even128, tot, 0.0), axis=1, keepdims=True)
        l_odd = jnp.sum(jnp.where(even128, 0.0, tot), axis=1, keepdims=True)
        stats = jnp.zeros((nb, 128), F32)
        for h, (vals, m, l) in enumerate(((pve, m_even, l_even), (pvo, m_odd, l_odd))):
            o = jnp.dot(pbuf[...], vals[...], preferred_element_type=F32)
            for g in range(2):
                j = 2 * h + g
                opart[r, :, pl.ds(j * hd, hd)] = o[g * nb:(g + 1) * nb]
                stats = jnp.where(lane == 2 * j, m[g * nb:(g + 1) * nb], stats)
                stats = jnp.where(lane == 2 * j + 1, l[g * nb:(g + 1) * nb], stats)
        opart[r, :, pl.ds(4 * hd, 128)] = stats

    def o_copy(g):
        lo, hi = GROUPS[g]
        part = pl.ds(lo, hi - lo)
        return pltpu.make_async_remote_copy(src_ref=opart.at[1, part], dst_ref=orecv.at[part], send_sem=osend.at[g],
                                            recv_sem=orecvs.at[g], device_id={'ctx': far}, device_id_type=MESH)

    row8 = lax.broadcasted_iota(jnp.int32, (8, rows), 0)
    col = lax.broadcasted_iota(jnp.int32, (8, rows), 1)
    same_head = lax.rem(col, 2) == lax.rem(row8 // 2, 2)
    slot_of = jnp.where(same_head, col // 2, 1 << 20)
    first = row8 < 4
    first128 = lax.broadcasted_iota(jnp.int32, (8, 128), 0) < 4
    first256 = lax.broadcasted_iota(jnp.int32, (8, 256), 0) < 4

    def scores(n, pair):
        at = pl.multiple_of((n * PER + 2 * pair) * 4, 8)
        slot = lax.rem(n, RING)
        q8 = jnp.concatenate([qrow[0, pl.ds(at, 8), :], qrow[1, pl.ds(at, 8), :]], axis=1).astype(BF16)
        out = []
        for u in (2 * pair, 2 * pair + 1):
            kk = jnp.concatenate([kring[slot, 0, u], kring[slot, 1, u]], axis=1)
            out.append(lax.dot_general(q8, kk, CONTRACT_LAST, preferred_element_type=F32))
        return jnp.where(first, out[0], out[1])

    def values(n, pair, s):
        i = n * PER + 2 * pair
        at = pl.multiple_of(i * 4, 8)
        slot = lax.rem(n, RING)
        ln = jnp.where(first128, lens_ref[i], lens_ref[i + 1])
        ln = jnp.concatenate([ln] * (rows // 128), axis=1)
        s = jnp.where(slot_of < ln, s, NEG)
        m = jnp.max(s, axis=1, keepdims=True)
        p = jnp.exp2((s - m) * factor)
        l = jnp.sum(p, axis=1, keepdims=True)
        pb = p.astype(BF16)
        out = []
        for u in (2 * pair, 2 * pair + 1):
            vv = jnp.concatenate([vring[slot, 0, u], vring[slot, 1, u]], axis=1)
            out.append(jnp.dot(pb, vv, preferred_element_type=F32))
        o = jnp.where(first256, out[0], out[1])
        osuf[0, pl.ds(at, 8), :] = o[:, :128]
        osuf[1, pl.ds(at, 8), :] = o[:, 128:]
        msuf[pl.ds(at, 8), :] = jnp.broadcast_to(m, (8, 128))
        lsuf[pl.ds(at, 8), :] = jnp.broadcast_to(l, (8, 128))

    pairs = range(PER // 2)
    blocks = nb // PER

    def first_scores():
        finish(kcopies(0))
        return tuple(scores(0, p) for p in pairs)

    def suffix(lo, hi, ss):
        lo, hi = lo // PER, hi // PER
        refill = hi + RING <= blocks
        assert refill or lo + RING >= blocks

        def body(n, ss):
            if refill:
                start(kcopies(n + RING))
            finish(kcopies(n + 1))
            finish(vcopies(n))
            nxt = tuple(scores(n + 1, p) for p in pairs)
            for p in pairs:
                values(n, p, ss[p])
            if refill:
                start(vcopies(n + RING))
            return nxt

        if hi < blocks:
            return lax.fori_loop(lo, hi, body, ss)
        ss = lax.fori_loop(lo, hi - 1, body, ss)
        finish(vcopies(hi - 1))
        for p in pairs:
            values(hi - 1, p, ss[p])

    half = width // 2
    mine = pl.ds(pl.multiple_of(head * half, 128), half)
    other = pl.ds(pl.multiple_of((1 - head) * half, 128), half)

    def y_copy(g):
        lo, hi = GROUPS[g]
        part = (pl.ds(lo, hi - lo), other if g < SPLIT else slice(None))
        return pltpu.make_async_remote_copy(src_ref=yown.at[part], dst_ref=yrecv.at[part], send_sem=ysend.at[g], recv_sem=yrecvs.at[g],
                                            device_id={'heads': 1 - head}, device_id_type=MESH)

    def f_copy(g):
        lo, hi = GROUPS[g]
        part = (pl.ds(lo, hi - lo), mine)
        return pltpu.make_async_remote_copy(src_ref=yfin.at[part], dst_ref=yfin.at[part], send_sem=fsend.at[g], recv_sem=frecv.at[g],
                                            device_id={'heads': 1 - head}, device_id_type=MESH)

    def finalize(g):
        y_copy(g).wait_recv()
        lo, hi = GROUPS[g]
        part = (pl.ds(lo, hi - lo), mine)
        yfin[part] = (x[part].astype(F32) + (yown[part] + yrecv[part])).astype(BF16)
        f_copy(g).start()

    def merge(g):
        o_copy(g).wait_recv()
        lo, hi = GROUPS[g]
        gsz = hi - lo
        part = pl.ds(lo, gsz)
        srcs = [opart.at[0], orecv]
        for j in range(4):
            rows_j = pl.ds(lo * 4 + j, gsz, stride=4)
            ms = [msuf[rows_j, :], snew[j, part, :]]
            for src in srcs:
                ms.append(jnp.broadcast_to(src[part, pl.ds(4 * hd + 2 * j, 1)], (gsz, 128)))
            top = functools.reduce(jnp.maximum, ms)
            ws = [jnp.exp2((m - top) * factor) for m in ms]
            den = ws[0] * lsuf[rows_j, :] + ws[1]
            for w, src in zip(ws[2:], srcs):
                den = den + w * src[part, pl.ds(4 * hd + 2 * j + 1, 1)]
            for d in range(2):
                at = j * hd + d * 128
                num = ws[0] * osuf[d, rows_j, :] + ws[1] * vnew[part, pl.ds((j // 2) * hd + d * 128, 128)]
                for w, src in zip(ws[2:], srcs):
                    num = num + w * src[part, pl.ds(at, 128)]
                att[pl.ds(0, gsz), pl.ds(at, 128)] = (num / den).astype(BF16)
        yown[part, :] = jnp.dot(att[pl.ds(0, gsz), :], wo[...], preferred_element_type=F32)
        y_copy(g).start()

    lens_copy.wait()
    ss = first_scores()
    ss = suffix(0, 8, ss)
    pv_share.wait_recv()
    split_values(1)
    pk_share.wait_recv()
    prefix(0)
    ss = suffix(8, 24, ss)
    q_copy.wait_recv()
    prefix(1)
    for g in range(len(GROUPS)):
        o_copy(g).start()
    ss = suffix(24, 40, ss)
    wo_copy.wait()
    merge(0)
    ss = suffix(40, 48, ss)
    merge(1)
    finalize(0)
    ss = suffix(48, 56, ss)
    merge(2)
    finalize(1)
    suffix(56, 64, ss)
    merge(3)
    finalize(2)
    q_copy.wait_send()
    pk_share.wait_send()
    pv_share.wait_send()
    for g, (lo, hi) in enumerate(GROUPS):
        o_copy(g).wait_send()
        y_copy(g).wait_send()
        part = pl.ds(lo, hi - lo)
        if g < SPLIT:
            f_copy(g).wait()
            y_ref[part, :] = yfin[part, :]
        else:
            y_copy(g).wait_recv()
            y_ref[part, :] = (x[part, :].astype(F32) + (yown[part, :] + yrecv[part, :])).astype(BF16)


def solution(mesh):
    row_spec = P(('dp', 'ctx'), None)
    col_spec = P(None, 'heads')
    pre_spec = P(('dp', 'ctx'), 'heads', None)
    suf_spec = P(('dp', 'ctx'), None, 'heads', None)

    def local_step(hidden, w_query, w_key, w_value, w_out, prefix_k, prefix_v, suffix_k, suffix_v, seq_lens):
        nb, width = hidden.shape
        qw = w_query.shape[1]
        kvw = w_key.shape[1]
        prows = 2 * prefix_k.shape[0]
        rows = 2 * suffix_k.shape[1]
        hbm_spec = pl.BlockSpec(memory_space=pltpu.HBM)
        dma = pltpu.SemaphoreType.DMA
        v = pltpu.VMEM
        return pl.pallas_call(
            step_kernel,
            out_shape=jax.ShapeDtypeStruct((nb, width), BF16),
            in_specs=[hbm_spec] * 10,
            out_specs=pl.BlockSpec(memory_space=pltpu.VMEM),
            scratch_shapes=[
                v((nb, width), BF16), v((width, qw), BF16), v((width, kvw), BF16), v((width, kvw), BF16), v((qw, width), BF16),
                v((2, 2, prows, 128), BF16), v((2, 2, prows, 128), BF16), v((2 * prows, 256), BF16), v((2 * prows, 256), BF16),
                v((RING, 2, PER, rows, 128), BF16), v((RING, 2, PER, rows, 128), BF16),
                v((4 * nb, 256), BF16), v((4 * nb, 256), BF16), v((2, 4 * nb, 128), F32), v((4, nb, 128), F32), v((nb, kvw), F32),
                v((2 * nb, 2 * prows), F32), v((2 * nb, 2 * prows), BF16),
                v((2, nb, qw + 128), F32), v((nb, qw + 128), F32),
                v((2, 4 * nb, 128), F32), v((4 * nb, 128), F32), v((4 * nb, 128), F32), v((nb // 2, qw), BF16),
                v((nb, width), F32), v((nb, width), F32), v((nb, width), BF16), pltpu.SMEM((nb,), jnp.int32),
                dma((10,)), dma((RING,)), dma((RING,)), dma((2,)), dma((2,)), dma((1,)), dma((1,)), dma((4,)), dma((4,)), dma((4,)), dma((4,)), dma((4,)), dma((4,)),
            ],
            compiler_params=pltpu.CompilerParams(collective_id=0, has_side_effects=True, vmem_limit_bytes=60 * 1024 * 1024),
        )(hidden, w_query, w_key, w_value, w_out, prefix_k, prefix_v, suffix_k, suffix_v, seq_lens)

    return jax.shard_map(local_step, mesh=mesh, in_specs=(row_spec, col_spec, col_spec, col_spec, P('heads', None), pre_spec, pre_spec, suf_spec, suf_spec, P(('dp', 'ctx'))), out_specs=row_spec, check_vma=False)
```
